32 devices in a mesh: row: 8 (over z, y), ta: 4 (over x, core).
Axes of the slice: x: 2, y: 2, z: 4, core: 2. Of those that a mesh axis runs over, the one named last changes fastest.
Arguments:
- hidden: bfloat16 [8, 256, 3584], P('row', None, 'ta'), may hold values from -6 to 6
- target: bfloat16 [8, 256, 3584], P('row', None, 'ta'), may hold values from -6 to 6
- w_down: bfloat16 [8, 2, 3584, 256], P('row', None, 'ta'), may hold values from -5 to 5
- w_up: bfloat16 [8, 2, 256, 3584], P('row', None, None, 'ta'), may hold values from -5 to 5
- m_down: float32 [8, 2, 3584, 256], P('row', None, 'ta'), may hold values from -9 to 9
- m_up: float32 [8, 2, 256, 3584], P('row', None, None, 'ta'), may hold values from -9 to 9
Outputs:
- avg_down: bfloat16 [2, 3584, 256], P(None, 'ta')
- avg_up: bfloat16 [2, 256, 3584], P(None, None, 'ta')
- mom_down: float32 [2, 3584, 256], P(None, 'ta')
- mom_up: float32 [2, 256, 3584], P(None, None, 'ta')
The draws below stay inside these ranges and needn't reach their ends.
All inputs are finite; a program needn't handle non-finite values.
Results may differ from the reference program's by a relative error of at most 0.019.
Values may be sent and summed in bfloat16 or wider, within the bound.
A program may use at most 128 MiB of HBM per device.

```python
import jax
import jax.numpy as jnp
from jax import lax

D = 3584
RANK = 256
LAYERS = 2
STEPS = 4
TOK = 256
REPLICAS = 8


def draw_hidden(key, part):
    values = jax.random.truncated_normal(jax.random.fold_in(key, 11), -6.0, 6.0, (REPLICAS, TOK, D), jnp.float32)
    return values.astype(jnp.bfloat16)


def draw_target(key, part):
    values = jax.random.truncated_normal(jax.random.fold_in(key, 12), -6.0, 6.0, (REPLICAS, TOK, D), jnp.float32)
    return values.astype(jnp.bfloat16)


def draw_w_down(key, part):
    values = jax.random.truncated_normal(jax.random.fold_in(key, 13), -5.0, 5.0, (REPLICAS, LAYERS, D, RANK), jnp.float32)
    return values.astype(jnp.bfloat16)


def draw_w_up(key, part):
    values = jax.random.truncated_normal(jax.random.fold_in(key, 14), -5.0, 5.0, (REPLICAS, LAYERS, RANK, D), jnp.float32)
    return values.astype(jnp.bfloat16)


def draw_m_down(key, part):
    values = 1.5 * jax.random.truncated_normal(jax.random.fold_in(key, 15), -6.0, 6.0, (REPLICAS, LAYERS, D, RANK), jnp.float32)
    return values.astype(jnp.float32)


def draw_m_up(key, part):
    values = 1.5 * jax.random.truncated_normal(jax.random.fold_in(key, 16), -6.0, 6.0, (REPLICAS, LAYERS, RANK, D), jnp.float32)
    return values.astype(jnp.float32)


def setup_inputs(seed: int = 0) -> dict:
    seeds = jax.random.split(jax.random.key(seed), 7)
    return {
        "hidden": draw_hidden(jax.random.fold_in(seeds[6], 71), 0),
        "target": draw_target(jax.random.fold_in(seeds[6], 71), 0),
        "w_down": draw_w_down(jax.random.fold_in(seeds[6], 71), 0),
        "w_up": draw_w_up(jax.random.fold_in(seeds[6], 71), 0),
        "m_down": draw_m_down(jax.random.fold_in(seeds[6], 71), 0),
        "m_up": draw_m_up(jax.random.fold_in(seeds[6], 71), 0),
    }


norm_eps = 1e-06
learn_rate = 0.02
moment_decay = 0.9

def silu_slope(preact):
    sigmoid_v = jax.nn.sigmoid(preact)
    return sigmoid_v * (1.0 + preact * (1.0 - sigmoid_v))

def replica_steps(hidden, target, w_down, w_up, m_down, m_up):
    for step_index in range(STEPS):
        stored = []
        current = hidden
        for layer_index in range(LAYERS):
            wide_rows = current.astype(jnp.float32)
            root_mean = jnp.sqrt(lax.optimization_barrier(jnp.mean(wide_rows * wide_rows, axis=1, keepdims=True)) + norm_eps)
            projected = jnp.dot(current, w_down[layer_index], preferred_element_type=jnp.float32) * D ** (-0.5)
            preact = projected / root_mean
            activation = jax.nn.silu(preact).astype(jnp.bfloat16)
            stored.append((current, root_mean, preact, activation))
            lifted = jnp.dot(activation, w_up[layer_index], preferred_element_type=jnp.float32) * RANK ** (-0.5)
            current = (wide_rows + lifted).astype(jnp.bfloat16)
        gradient = current.astype(jnp.float32) - target.astype(jnp.float32)
        grads_down = [None] * LAYERS
        grads_up = [None] * LAYERS
        for layer_index in reversed(range(LAYERS)):
            current, root_mean, preact, activation = stored[layer_index]
            grad_low = gradient.astype(jnp.bfloat16)
            grads_up[layer_index] = jnp.dot(activation.T, grad_low, preferred_element_type=jnp.float32) * RANK ** (-0.5)
            grad_act = jnp.dot(grad_low, w_up[layer_index].T, preferred_element_type=jnp.float32) * RANK ** (-0.5)
            grad_pre = grad_act * silu_slope(preact)
            row_dot = lax.optimization_barrier(jnp.sum(grad_pre * preact, axis=1, keepdims=True))
            grad_proj = (grad_pre / root_mean).astype(jnp.bfloat16)
            grads_down[layer_index] = jnp.dot(current.T, grad_proj, preferred_element_type=jnp.float32) * D ** (-0.5)
            wide_rows = current.astype(jnp.float32)
            through = jnp.dot(grad_proj, w_down[layer_index].T, preferred_element_type=jnp.float32) * D ** (-0.5)
            gradient = gradient + through - row_dot * wide_rows / (D * root_mean * root_mean)
        m_down = moment_decay * m_down + jnp.stack(grads_down)
        m_up = moment_decay * m_up + jnp.stack(grads_up)
        w_down = (w_down.astype(jnp.float32) - learn_rate * m_down).astype(jnp.bfloat16)
        w_up = (w_up.astype(jnp.float32) - learn_rate * m_up).astype(jnp.bfloat16)
    return (w_down, w_up, m_down, m_up)

def accumulate(totals, inputs):
    finals = replica_steps(inputs[0], inputs[1], inputs[2], inputs[3], inputs[4], inputs[5])
    return (tuple((total + final.astype(jnp.float32) for total, final in zip(totals, finals))), None)

def reference(hidden, target, w_down, w_up, m_down, m_up):
    replicas = hidden.shape[0]
    zeros_init = (jnp.zeros(w_down.shape[1:], jnp.float32), jnp.zeros(w_up.shape[1:], jnp.float32), jnp.zeros(m_down.shape[1:], jnp.float32), jnp.zeros(m_up.shape[1:], jnp.float32))
    totals, unused = lax.scan(accumulate, zeros_init, (hidden, target, w_down, w_up, m_down, m_up))
    avg_down = (totals[0] / replicas).astype(jnp.bfloat16)
    avg_up = (totals[1] / replicas).astype(jnp.bfloat16)
    return (avg_down, avg_up, totals[2] / replicas, totals[3] / replicas)
```

```python
import functools

import jax
import jax.numpy as jnp
from jax import lax
from jax.experimental import pallas as pl
from jax.experimental.pallas import tpu as pltpu
from jax.sharding import PartitionSpec as P

MESH = pl.DeviceIdType.MESH
STEPS = 4
norm_eps = 1e-06
learn_rate = 0.02
moment_decay = 0.9


def dot_nn(a, b):
    return jnp.dot(a, b, preferred_element_type=jnp.float32)


def dot_nt(a, b):
    return lax.dot_general(a, b, (((1,), (1,)), ((), ())), preferred_element_type=jnp.float32)


def local_kernel(
    shards,
    x0_ref, tg_ref, wd_in, wu_in, md_in, mu_in,
    wd, wu, md_out, mu_out,
    md, mu, x1, xt, gr, pre, act, inv, tot, sqs, low,
    s1, r1, s2, r2, s3, r3, q1, p1, q2, p2, q3, p3,
    main_send, main_recv, side_send, side_recv,
):
    tok, width = x0_ref.shape
    rank = wd.shape[2]
    full = width * shards
    half = tok // 2
    chips = shards // 2
    me = lax.axis_index("ta")
    core = lax.rem(me, 2)
    sibling = me + 1 - 2 * core
    partners = [lax.rem(me + 2 * k, shards) for k in range(1, chips)]
    d_scale = full ** (-0.5)
    r_scale = rank ** (-0.5)

    barrier = pltpu.get_barrier_semaphore()
    for peer in [sibling] + partners:
        pl.semaphore_signal(barrier, inc=1, device_id={"ta": peer}, device_id_type=MESH)
    pl.semaphore_wait(barrier, chips)

    wd[...] = wd_in[...]
    wu[...] = wu_in[...]
    md[...] = md_in[...]
    mu[...] = mu_in[...]

    mine = pl.ds(pl.multiple_of(core * half, half), half)
    other = pl.ds(pl.multiple_of((1 - core) * half, half), half)

    def send(src, dst, sems, index, peer):
        copy = pltpu.make_async_remote_copy(
            src_ref=src, dst_ref=dst,
            send_sem=sems[0].at[index], recv_sem=sems[1].at[index],
            device_id={"ta": peer}, device_id_type=MESH,
        )
        copy.start()
        return copy

    main = (main_send, main_recv)
    side = (side_send, side_recv)

    def to_row(column):
        return jnp.broadcast_to(column, (half, half)).T[0:8]

    def to_column(row):
        return jnp.broadcast_to(row[0:1, :], (half, half)).T[:, 0:1]

    def exchange(parity, value, squares, work):
        tot[...] = value
        s1[...] = tot[other, :].astype(jnp.bfloat16)
        copies = [send(s1, r1, main, 0, sibling)]
        if squares is not None:
            sqs[...] = squares
            q1[...] = to_row(sqs[other, :])
            copies.append(send(q1, p1, side, 0, sibling))
            own_row = to_row(sqs[mine, :])
        for copy in copies:
            copy.wait()
        pair = tot[mine, :] + r1[...].astype(jnp.float32)
        s2[...] = pair.astype(jnp.bfloat16)
        base = parity * (chips - 1)
        copies = [
            send(s2, r2.at[base + k], main, 1 + base + k, peer) for k, peer in enumerate(partners)
        ]
        if squares is not None:
            pair_row = own_row + p1[...]
            q2[...] = pair_row
            copies += [
                send(q2, p2.at[base + k], side, 1 + base + k, peer)
                for k, peer in enumerate(partners)
            ]
        if work is not None:
            work()
        for copy in copies:
            copy.wait()
        total = pair
        for k in range(chips - 1):
            total = total + r2[base + k].astype(jnp.float32)
        last = 1 + 2 * (chips - 1)
        s3[...] = total.astype(jnp.bfloat16)
        copies = [send(s3, r3, main, last, sibling)]
        tot[mine, :] = total
        if squares is not None:
            row = pair_row
            for k in range(chips - 1):
                row = row + p2[base + k]
            q3[...] = row
            copies.append(send(q3, p3, side, last, sibling))
            sqs[mine, :] = to_column(row)
        for copy in copies:
            copy.wait()
        tot[other, :] = r3[...].astype(jnp.float32)
        if squares is not None:
            sqs[other, :] = to_column(p3[...])

    def forward(layer, rows, wide_rows):
        squares = jnp.sum(wide_rows * wide_rows, axis=1, keepdims=True)
        exchange(layer, dot_nn(rows, wd[layer]) * d_scale, squares, None)
        inverse = lax.rsqrt(sqs[...] / full + norm_eps)
        preact = tot[...] * inverse
        activation = (preact * jax.nn.sigmoid(preact)).astype(jnp.bfloat16)
        inv[layer] = inverse
        pre[layer] = preact
        act[layer] = activation
        lifted = dot_nn(activation, wu[layer]) * r_scale
        return (wide_rows + lifted).astype(jnp.bfloat16)

    def update(w, m, layer, grad):
        moment = moment_decay * m[layer] + grad
        m[layer] = moment
        w[layer] = (w[layer].astype(jnp.float32) - learn_rate * moment).astype(jnp.bfloat16)

    def update_up(layer):
        update(wu, mu, layer, dot_nn(act[layer].T, gr[...].astype(jnp.bfloat16)) * r_scale)

    def low_grads(layer):
        preact = pre[layer]
        sig = jax.nn.sigmoid(preact)
        grad_pre = tot[...] * (sig * (1.0 + preact * (1.0 - sig)))
        low[...] = (grad_pre * inv[layer]).astype(jnp.bfloat16)
        return jnp.sum(grad_pre * preact, axis=1, keepdims=True)

    def step(index, carry):
        x1[...] = forward(0, x0_ref[...], x0_ref[...].astype(jnp.float32))
        outcome = forward(1, x1[...], x1[...].astype(jnp.float32))
        gr[...] = outcome.astype(jnp.float32) - tg_ref[...].astype(jnp.float32)

        partial_act = dot_nt(gr[...].astype(jnp.bfloat16), wu[1]) * r_scale
        exchange(0, partial_act, None, lambda: update_up(1))
        row_dot = low_grads(1)
        through = dot_nt(low[...], wd[1]) * d_scale
        coefficient = row_dot * inv[1] * inv[1] / full
        gr[...] = gr[...] + through - coefficient * x1[...].astype(jnp.float32)

        def work():
            update(wd, md, 1, dot_nn(x1[...].T, low[...]) * d_scale)
            update_up(0)

        partial_act = dot_nt(gr[...].astype(jnp.bfloat16), wu[0]) * r_scale
        exchange(1, partial_act, None, work)
        low_grads(0)
        update(wd, md, 0, dot_nn(xt[...], low[...]) * d_scale)
        return carry

    xt[...] = x0_ref[...].T
    lax.fori_loop(0, STEPS, step, 0)
    md_out[...] = md[...].astype(jnp.bfloat16)
    mu_out[...] = mu[...].astype(jnp.bfloat16)


def local_steps(shards, hidden, target, w_down, w_up, m_down, m_up):
    tok, width = hidden.shape
    layers, _, rank = w_down.shape
    half = tok // 2
    hops = shards // 2 - 1
    bf, f32 = jnp.bfloat16, jnp.float32
    vmem = pl.BlockSpec(memory_space=pltpu.VMEM)
    sems = 2 + 2 * hops
    return pl.pallas_call(
        functools.partial(local_kernel, shards),
        out_shape=[
            jax.ShapeDtypeStruct(w_down.shape, bf),
            jax.ShapeDtypeStruct(w_up.shape, bf),
            jax.ShapeDtypeStruct(m_down.shape, bf),
            jax.ShapeDtypeStruct(m_up.shape, bf),
        ],
        in_specs=[vmem] * 6,
        out_specs=[vmem] * 4,
        scratch_shapes=[
            pltpu.VMEM(m_down.shape, f32),
            pltpu.VMEM(m_up.shape, f32),
            pltpu.VMEM((tok, width), bf),
            pltpu.VMEM((width, tok), bf),
            pltpu.VMEM((tok, width), f32),
            pltpu.VMEM((layers, tok, rank), f32),
            pltpu.VMEM((layers, tok, rank), bf),
            pltpu.VMEM((layers, tok, 1), f32),
            pltpu.VMEM((tok, rank), f32),
            pltpu.VMEM((tok, 1), f32),
            pltpu.VMEM((tok, rank), bf),
            pltpu.VMEM((half, rank), bf),
            pltpu.VMEM((half, rank), bf),
            pltpu.VMEM((half, rank), bf),
            pltpu.VMEM((2 * hops, half, rank), bf),
            pltpu.VMEM((half, rank), bf),
            pltpu.VMEM((half, rank), bf),
            pltpu.VMEM((8, half), f32),
            pltpu.VMEM((8, half), f32),
            pltpu.VMEM((8, half), f32),
            pltpu.VMEM((2 * hops, 8, half), f32),
            pltpu.VMEM((8, half), f32),
            pltpu.VMEM((8, half), f32),
            pltpu.SemaphoreType.DMA((sems,)),
            pltpu.SemaphoreType.DMA((sems,)),
            pltpu.SemaphoreType.DMA((sems,)),
            pltpu.SemaphoreType.DMA((sems,)),
        ],
        compiler_params=pltpu.CompilerParams(
            collective_id=0, has_side_effects=True, vmem_limit_bytes=60 * 1024 * 1024
        ),
    )(hidden, target, w_down, w_up, m_down, m_up)


def body(shards, replicas, hidden, target, w_down, w_up, m_down, m_up):
    states = local_steps(
        shards, hidden[0], target[0], w_down[0], w_up[0], m_down[0], m_up[0]
    )
    totals = lax.psum(tuple(states), "row")
    scale = 1.0 / replicas
    means = [total.astype(jnp.float32) * scale for total in totals]
    return (
        means[0].astype(jnp.bfloat16),
        means[1].astype(jnp.bfloat16),
        means[2],
        means[3],
    )


def solution(mesh):
    placed = (
        P("row", None, "ta"),
        P("row", None, "ta"),
        P("row", None, "ta", None),
        P("row", None, None, "ta"),
        P("row", None, "ta", None),
        P("row", None, None, "ta"),
    )
    return jax.shard_map(
        functools.partial(body, mesh.shape["ta"], mesh.shape["row"]),
        mesh=mesh,
        in_specs=placed,
        out_specs=(
            P(None, "ta", None),
            P(None, None, "ta"),
            P(None, "ta", None),
            P(None, None, "ta"),
        ),
        check_vma=False,
    )
```

```python
import functools

import jax
import jax.numpy as jnp
from jax import lax
from jax.experimental import pallas as pl
from jax.experimental.pallas import tpu as pltpu
from jax.sharding import PartitionSpec as P

MESH = pl.DeviceIdType.MESH
STEPS = 4
norm_eps = 1e-06
learn_rate = 0.02
moment_decay = 0.9


def dot_nn(a, b):
    return jnp.dot(a, b, preferred_element_type=jnp.float32)


def dot_nt(a, b):
    return lax.dot_general(a, b, (((1,), (1,)), ((), ())), preferred_element_type=jnp.float32)


def row_bits(replicas, *lengths):
    if replicas & (replicas - 1) or any(length % (16 * replicas) for length in lengths):
        return []
    return [2**k for k in range(replicas.bit_length() - 1)]


def fused_kernel(
    shards, replicas,
    x0_ref, tg_ref, wd_in, wu_in, md_in, mu_in,
    wd_out, wu_out, md_out, mu_out,
    wd, wu, md, mu, mdl, mul, res_wd, res_wu, res_md, res_mu,
    got_wd, got_wu, got_md, got_mu, row_send, row_recv,
    x1, xt, gr, pre, act, inv, tot, sqs, low,
    s1, r1, s2, r2, s3, r3, q1, p1, q2, p2, q3, p3,
    main_send, main_recv, side_send, side_recv,
):
    tok, width = x0_ref.shape
    rank = wd.shape[2]
    full = width * shards
    half = tok // 2
    chips = shards // 2
    me = lax.axis_index("ta")
    core = lax.rem(me, 2)
    sibling = me + 1 - 2 * core
    partners = [lax.rem(me + 2 * k, shards) for k in range(1, chips)]
    d_scale = full ** (-0.5)
    r_scale = rank ** (-0.5)

    barrier = pltpu.get_barrier_semaphore()
    for peer in [sibling] + partners:
        pl.semaphore_signal(barrier, inc=1, device_id={"ta": peer}, device_id_type=MESH)
    bits = row_bits(replicas, width, rank)
    levels = len(bits)
    spot = lax.axis_index("row")
    own_bit = {bit: lax.rem(spot // bit, 2) for bit in bits}
    row_peer = {bit: spot + bit - 2 * bit * own_bit[bit] for bit in bits}
    for bit in bits:
        pl.semaphore_signal(barrier, inc=1, device_id={"row": row_peer[bit]}, device_id_type=MESH)
    pl.semaphore_wait(barrier, chips + levels)

    wd[...] = wd_in[...]
    wu[...] = wu_in[...]
    md[...] = md_in[...]
    mu[...] = mu_in[...]

    mine = pl.ds(pl.multiple_of(core * half, half), half)
    other = pl.ds(pl.multiple_of((1 - core) * half, half), half)

    def send(src, dst, sems, index, peer):
        copy = pltpu.make_async_remote_copy(
            src_ref=src, dst_ref=dst,
            send_sem=sems[0].at[index], recv_sem=sems[1].at[index],
            device_id={"ta": peer}, device_id_type=MESH,
        )
        copy.start()
        return copy

    main = (main_send, main_recv)
    side = (side_send, side_recv)

    def to_row(column):
        return jnp.broadcast_to(column, (half, half)).T[0:8]

    def to_column(row):
        return jnp.broadcast_to(row[0:1, :], (half, half)).T[:, 0:1]

    def exchange(parity, value, squares, work):
        tot[...] = value
        s1[...] = tot[other, :].astype(jnp.bfloat16)
        copies = [send(s1, r1, main, 0, sibling)]
        if squares is not None:
            sqs[...] = squares
            q1[...] = to_row(sqs[other, :])
            copies.append(send(q1, p1, side, 0, sibling))
            own_row = to_row(sqs[mine, :])
        for copy in copies:
            copy.wait()
        pair = tot[mine, :] + r1[...].astype(jnp.float32)
        s2[...] = pair.astype(jnp.bfloat16)
        base = parity * (chips - 1)
        copies = [
            send(s2, r2.at[base + k], main, 1 + base + k, peer) for k, peer in enumerate(partners)
        ]
        if squares is not None:
            pair_row = own_row + p1[...]
            q2[...] = pair_row
            copies += [
                send(q2, p2.at[base + k], side, 1 + base + k, peer)
                for k, peer in enumerate(partners)
            ]
        if work is not None:
            work()
        for copy in copies:
            copy.wait()
        total = pair
        for k in range(chips - 1):
            total = total + r2[base + k].astype(jnp.float32)
        last = 1 + 2 * (chips - 1)
        s3[...] = total.astype(jnp.bfloat16)
        copies = [send(s3, r3, main, last, sibling)]
        tot[mine, :] = total
        if squares is not None:
            row = pair_row
            for k in range(chips - 1):
                row = row + p2[base + k]
            q3[...] = row
            copies.append(send(q3, p3, side, last, sibling))
            sqs[mine, :] = to_column(row)
        for copy in copies:
            copy.wait()
        tot[other, :] = r3[...].astype(jnp.float32)
        if squares is not None:
            sqs[other, :] = to_column(p3[...])

    def forward(layer, rows, wide_rows):
        squares = jnp.sum(wide_rows * wide_rows, axis=1, keepdims=True)
        exchange(layer, dot_nn(rows, wd[layer]) * d_scale, squares, None)
        inverse = lax.rsqrt(sqs[...] / full + norm_eps)
        preact = tot[...] * inverse
        activation = (preact * jax.nn.sigmoid(preact)).astype(jnp.bfloat16)
        inv[layer] = inverse
        pre[layer] = preact
        act[layer] = activation
        lifted = dot_nn(activation, wu[layer]) * r_scale
        return (wide_rows + lifted).astype(jnp.bfloat16)

    def update(w, m, layer, grad):
        moment = moment_decay * m[layer] + grad
        m[layer] = moment
        w[layer] = (w[layer].astype(jnp.float32) - learn_rate * moment).astype(jnp.bfloat16)

    def update_up(layer):
        update(wu, mu, layer, dot_nn(act[layer].T, gr[...].astype(jnp.bfloat16)) * r_scale)

    def low_grads(layer):
        preact = pre[layer]
        sig = jax.nn.sigmoid(preact)
        grad_pre = tot[...] * (sig * (1.0 + preact * (1.0 - sig)))
        low[...] = (grad_pre * inv[layer]).astype(jnp.bfloat16)
        return jnp.sum(grad_pre * preact, axis=1, keepdims=True)

    plain = list(bits)
    swapped = plain[:2][::-1] + plain[2:]
    down, up = (wd, got_wd, res_wd), (wu, got_wu, res_wu)
    mdown, mup = (mdl, got_md, res_md), (mul, got_mu, res_mu)
    chunks = []
    for layer in reversed(range(wd.shape[0])):
        for group in ((up, mup), (down, mdown)):
            for triple in group:
                order = swapped if len(chunks) in (1, 4) else plain
                chunks.append(triple + (layer, order))
    late = [k for k, entry in enumerate(chunks) if entry[3] == 0 and (entry[0] is wd or entry[0] is mdl)]
    early = [k for k in range(len(chunks)) if k not in late]

    def region(chunk, depth):
        acc, _, _, _, order = chunks[chunk]
        start = 0
        for k in range(depth):
            start = start + own_bit[order[k]] * (acc.shape[1] >> (k + 1))
        return pl.multiple_of(start, acc.shape[1] >> depth) if depth else 0

    def row_copy(chunk, stage):
        acc, got, res, layer, order = chunks[chunk]
        rows = acc.shape[1]
        if stage < levels:
            bit = order[stage]
            size = rows >> (stage + 1)
            away = region(chunk, stage) + (1 - own_bit[bit]) * size
            src = acc.at[layer, pl.ds(pl.multiple_of(away, size), size)]
            dst = got.at[layer, pl.ds(rows - 2 * size, size)]
        else:
            depth = 2 * levels - stage
            bit = order[depth - 1]
            part = pl.ds(region(chunk, depth), rows >> depth)
            src = dst = res.at[layer, part]
        index = chunk * 2 * levels + stage
        return pltpu.make_async_remote_copy(
            src_ref=src, dst_ref=dst,
            send_sem=row_send.at[index], recv_sem=row_recv.at[index],
            device_id={"row": row_peer[bit]}, device_id_type=MESH,
        )

    def step(index, carry):
        x1[...] = forward(0, x0_ref[...], x0_ref[...].astype(jnp.float32))
        outcome = forward(1, x1[...], x1[...].astype(jnp.float32))
        gr[...] = outcome.astype(jnp.float32) - tg_ref[...].astype(jnp.float32)

        partial_act = dot_nt(gr[...].astype(jnp.bfloat16), wu[1]) * r_scale
        exchange(0, partial_act, None, lambda: update_up(1))
        row_dot = low_grads(1)
        through = dot_nt(low[...], wd[1]) * d_scale
        coefficient = row_dot * inv[1] * inv[1] / full
        gr[...] = gr[...] + through - coefficient * x1[...].astype(jnp.float32)

        def work():
            update(wd, md, 1, dot_nn(x1[...].T, low[...]) * d_scale)
            update_up(0)

            @pl.when(index == STEPS - 1)
            def _():
                mul[...] = mu[...].astype(jnp.bfloat16)
                mdl[1] = md[1].astype(jnp.bfloat16)
                for chunk in early if levels else []:
                    row_copy(chunk, 0).start()

        partial_act = dot_nt(gr[...].astype(jnp.bfloat16), wu[0]) * r_scale
        exchange(1, partial_act, None, work)
        low_grads(0)
        update(wd, md, 0, dot_nn(xt[...], low[...]) * d_scale)
        return carry

    xt[...] = x0_ref[...].T
    lax.fori_loop(0, STEPS, step, 0)
    mdl[0] = md[0].astype(jnp.bfloat16)
    if not levels:
        wd_out[...] = wd[...]
        wu_out[...] = wu[...]
        md_out[...] = mdl[...]
        mu_out[...] = mul[...]
        return
    for chunk in late:
        row_copy(chunk, 0).start()

    count = len(chunks)
    for slot in range(count + 2 * levels - 1):
        for chunk in range(count):
            stage = slot - chunk
            if stage < 0 or stage >= 2 * levels:
                continue
            row_copy(chunk, stage).wait_recv()
            if stage < levels:
                acc, got, res, layer, order = chunks[chunk]
                size = acc.shape[1] >> (stage + 1)
                keep = pl.ds(region(chunk, stage + 1), size)
                landed = got.at[layer, pl.ds(acc.shape[1] - 2 * size, size)]
                total = acc[layer, keep, :].astype(jnp.float32) + landed[...].astype(jnp.float32)
                if stage < levels - 1:
                    acc[layer, keep, :] = total.astype(jnp.bfloat16)
                else:
                    res[layer, keep, :] = (total * (1.0 / replicas)).astype(jnp.bfloat16)
            if stage < 2 * levels - 1:
                row_copy(chunk, stage + 1).start()
    for chunk in range(count):
        for stage in range(2 * levels):
            row_copy(chunk, stage).wait_send()
    wd_out[...] = res_wd[...]
    wu_out[...] = res_wu[...]
    md_out[...] = res_md[...]
    mu_out[...] = res_mu[...]


def fused(shards, replicas, hidden, target, w_down, w_up, m_down, m_up):
    tok, width = hidden.shape
    layers, _, rank = w_down.shape
    half = tok // 2
    hops = shards // 2 - 1
    bf, f32 = jnp.bfloat16, jnp.float32
    vmem = pl.BlockSpec(memory_space=pltpu.VMEM)
    sems = 2 + 2 * hops
    row_sems = max(1, 4 * layers * 2 * len(row_bits(replicas, width, rank)))
    return pl.pallas_call(
        functools.partial(fused_kernel, shards, replicas),
        out_shape=[
            jax.ShapeDtypeStruct(w_down.shape, bf),
            jax.ShapeDtypeStruct(w_up.shape, bf),
            jax.ShapeDtypeStruct(m_down.shape, bf),
            jax.ShapeDtypeStruct(m_up.shape, bf),
        ],
        in_specs=[vmem] * 6,
        out_specs=[vmem] * 4,
        scratch_shapes=[
            pltpu.VMEM(w_down.shape, bf),
            pltpu.VMEM(w_up.shape, bf),
            pltpu.VMEM(m_down.shape, f32),
            pltpu.VMEM(m_up.shape, f32),
            pltpu.VMEM(m_down.shape, bf),
            pltpu.VMEM(m_up.shape, bf),
            pltpu.VMEM(w_down.shape, bf),
            pltpu.VMEM(w_up.shape, bf),
            pltpu.VMEM(m_down.shape, bf),
            pltpu.VMEM(m_up.shape, bf),
            pltpu.VMEM(w_down.shape, bf),
            pltpu.VMEM(w_up.shape, bf),
            pltpu.VMEM(m_down.shape, bf),
            pltpu.VMEM(m_up.shape, bf),
            pltpu.SemaphoreType.DMA((row_sems,)),
            pltpu.SemaphoreType.DMA((row_sems,)),
            pltpu.VMEM((tok, width), bf),
            pltpu.VMEM((width, tok), bf),
            pltpu.VMEM((tok, width), f32),
            pltpu.VMEM((layers, tok, rank), f32),
            pltpu.VMEM((layers, tok, rank), bf),
            pltpu.VMEM((layers, tok, 1), f32),
            pltpu.VMEM((tok, rank), f32),
            pltpu.VMEM((tok, 1), f32),
            pltpu.VMEM((tok, rank), bf),
            pltpu.VMEM((half, rank), bf),
            pltpu.VMEM((half, rank), bf),
            pltpu.VMEM((half, rank), bf),
            pltpu.VMEM((2 * hops, half, rank), bf),
            pltpu.VMEM((half, rank), bf),
            pltpu.VMEM((half, rank), bf),
            pltpu.VMEM((8, half), f32),
            pltpu.VMEM((8, half), f32),
            pltpu.VMEM((8, half), f32),
            pltpu.VMEM((2 * hops, 8, half), f32),
            pltpu.VMEM((8, half), f32),
            pltpu.VMEM((8, half), f32),
            pltpu.SemaphoreType.DMA((sems,)),
            pltpu.SemaphoreType.DMA((sems,)),
            pltpu.SemaphoreType.DMA((sems,)),
            pltpu.SemaphoreType.DMA((sems,)),
        ],
        compiler_params=pltpu.CompilerParams(
            collective_id=0, has_side_effects=True, vmem_limit_bytes=60 * 1024 * 1024
        ),
    )(hidden, target, w_down, w_up, m_down, m_up)


def body(shards, replicas, hidden, target, w_down, w_up, m_down, m_up):
    means = fused(
        shards, replicas, hidden[0], target[0], w_down[0], w_up[0], m_down[0], m_up[0]
    )
    if not row_bits(replicas, hidden.shape[2], w_down.shape[3]):
        totals = lax.psum(tuple(means), "row")
        means = [total.astype(jnp.float32) / replicas for total in totals]
    return (
        means[0].astype(jnp.bfloat16),
        means[1].astype(jnp.bfloat16),
        means[2].astype(jnp.float32),
        means[3].astype(jnp.float32),
    )


def solution(mesh):
    placed = (
        P("row", None, "ta"),
        P("row", None, "ta"),
        P("row", None, "ta", None),
        P("row", None, None, "ta"),
        P("row", None, "ta", None),
        P("row", None, None, "ta"),
    )
    return jax.shard_map(
        functools.partial(body, mesh.shape["ta"], mesh.shape["row"]),
        mesh=mesh,
        in_specs=placed,
        out_specs=(
            P(None, "ta", None),
            P(None, None, "ta"),
            P(None, "ta", None),
            P(None, None, "ta"),
        ),
        check_vma=False,
    )
```

```python
import functools

import jax
import jax.numpy as jnp
from jax import lax
from jax.experimental import pallas as pl
from jax.experimental.pallas import tpu as pltpu
from jax.sharding import PartitionSpec as P

MESH = pl.DeviceIdType.MESH
STEPS = 4
norm_eps = 1e-06
learn_rate = 0.02
moment_decay = 0.9


def dot_nn(a, b):
    return jnp.dot(a, b, preferred_element_type=jnp.float32)


def dot_nt(a, b):
    return lax.dot_general(a, b, (((1,), (1,)), ((), ())), preferred_element_type=jnp.float32)


def row_bits(replicas, *lengths):
    if replicas & (replicas - 1) or any(length % (16 * replicas) for length in lengths):
        return []
    return [2**k for k in range(replicas.bit_length() - 1)]


def fused_kernel(
    shards, replicas,
    x0_ref, tg_ref, wd_in, wu_in, md_in, mu_in,
    wd_out, wu_out, md_out, mu_out,
    wd, wu, md, mu, wdl, wul, mdl, mul, res_wd, res_wu, res_md, res_mu,
    got_wd, got_wu, got_md, got_mu, row_send, row_recv,
    x1, xt, gr, pre, act, inv, tot, sqs, low,
    s1, r1, s2, r2, s3, r3, q1, p1, q2, p2, q3, p3,
    main_send, main_recv, side_send, side_recv,
):
    tok, width = x0_ref.shape
    rank = wd.shape[2]
    full = width * shards
    half = tok // 2
    chips = shards // 2
    me = lax.axis_index("ta")
    core = lax.rem(me, 2)
    sibling = me + 1 - 2 * core
    partners = [lax.rem(me + 2 * k, shards) for k in range(1, chips)]
    d_scale = full ** (-0.5)
    r_scale = rank ** (-0.5)

    barrier = pltpu.get_barrier_semaphore()
    for peer in [sibling] + partners:
        pl.semaphore_signal(barrier, inc=1, device_id={"ta": peer}, device_id_type=MESH)
    bits = row_bits(replicas, width, rank)
    levels = len(bits)
    spot = lax.axis_index("row")
    own_bit = {bit: lax.rem(spot // bit, 2) for bit in bits}
    row_peer = {bit: spot + bit - 2 * bit * own_bit[bit] for bit in bits}
    for bit in bits:
        pl.semaphore_signal(barrier, inc=1, device_id={"row": row_peer[bit]}, device_id_type=MESH)
    pl.semaphore_wait(barrier, chips + levels)

    wd[...] = wd_in[...]
    wu[...] = wu_in[...]
    md[...] = md_in[...]
    mu[...] = mu_in[...]

    mine = pl.ds(pl.multiple_of(core * half, half), half)
    other = pl.ds(pl.multiple_of((1 - core) * half, half), half)

    def send(src, dst, sems, index, peer):
        copy = pltpu.make_async_remote_copy(
            src_ref=src, dst_ref=dst,
            send_sem=sems[0].at[index], recv_sem=sems[1].at[index],
            device_id={"ta": peer}, device_id_type=MESH,
        )
        copy.start()
        return copy

    main = (main_send, main_recv)
    side = (side_send, side_recv)

    def to_row(column):
        return jnp.broadcast_to(column, (half, half)).T[0:8]

    def to_column(row):
        return jnp.broadcast_to(row[0:1, :], (half, half)).T[:, 0:1]

    def exchange(parity, value, squares, work):
        tot[...] = value
        s1[...] = tot[other, :].astype(jnp.bfloat16)
        copies = [send(s1, r1, main, 0, sibling)]
        if squares is not None:
            sqs[...] = squares
            q1[...] = to_row(sqs[other, :])
            copies.append(send(q1, p1, side, 0, sibling))
            own_row = to_row(sqs[mine, :])
        for copy in copies:
            copy.wait()
        pair = tot[mine, :] + r1[...].astype(jnp.float32)
        s2[...] = pair.astype(jnp.bfloat16)
        base = parity * (chips - 1)
        copies = [
            send(s2, r2.at[base + k], main, 1 + base + k, peer) for k, peer in enumerate(partners)
        ]
        if squares is not None:
            pair_row = own_row + p1[...]
            q2[...] = pair_row
            copies += [
                send(q2, p2.at[base + k], side, 1 + base + k, peer)
                for k, peer in enumerate(partners)
            ]
        if work is not None:
            work()
        for copy in copies:
            copy.wait()
        total = pair
        for k in range(chips - 1):
            total = total + r2[base + k].astype(jnp.float32)
        last = 1 + 2 * (chips - 1)
        s3[...] = total.astype(jnp.bfloat16)
        copies = [send(s3, r3, main, last, sibling)]
        tot[mine, :] = total
        if squares is not None:
            row = pair_row
            for k in range(chips - 1):
                row = row + p2[base + k]
            q3[...] = row
            copies.append(send(q3, p3, side, last, sibling))
            sqs[mine, :] = to_column(row)
        for copy in copies:
            copy.wait()
        tot[other, :] = r3[...].astype(jnp.float32)
        if squares is not None:
            sqs[other, :] = to_column(p3[...])

    def forward(layer, rows, wide_rows):
        squares = jnp.sum(wide_rows * wide_rows, axis=1, keepdims=True)
        exchange(layer, dot_nn(rows, wd[layer]) * d_scale, squares, None)
        inverse = lax.rsqrt(sqs[...] / full + norm_eps)
        preact = tot[...] * inverse
        activation = (preact * jax.nn.sigmoid(preact)).astype(jnp.bfloat16)
        inv[layer] = inverse
        pre[layer] = preact
        act[layer] = activation
        lifted = dot_nn(activation, wu[layer]) * r_scale
        return (wide_rows + lifted).astype(jnp.bfloat16)

    def update(w, m, layer, grad, last):
        moment = moment_decay * m[layer] + grad
        m[layer] = moment
        if last and levels:
            return
        w[layer] = (w[layer].astype(jnp.float32) - learn_rate * moment).astype(jnp.bfloat16)

    def update_up(layer, last):
        update(wu, mu, layer, dot_nn(act[layer].T, gr[...].astype(jnp.bfloat16)) * r_scale, last)

    def low_grads(layer):
        preact = pre[layer]
        sig = jax.nn.sigmoid(preact)
        grad_pre = tot[...] * (sig * (1.0 + preact * (1.0 - sig)))
        low[...] = (grad_pre * inv[layer]).astype(jnp.bfloat16)
        return jnp.sum(grad_pre * preact, axis=1, keepdims=True)

    down, up = (wdl, got_wd, res_wd), (wul, got_wu, res_wu)
    mdown, mup = (mdl, got_md, res_md), (mul, got_mu, res_mu)
    layers = list(reversed(range(wd.shape[0])))
    chunks = [pair + (layer, bits) for layer in layers for pair in (up, down)]
    first = len(chunks)
    chunks += [pair + (layer, bits) for layer in layers for pair in (mup, mdown)]

    def start(picked):
        for chunk in picked if levels else []:
            row_copy(chunk, 0).start()

    def advance(slot):
        for chunk in range(len(chunks)):
            stage = slot - chunk
            if not levels or stage < 0 or stage >= 2 * levels:
                continue
            row_copy(chunk, stage).wait_recv()
            if stage < levels:
                acc, got, res, layer, order = chunks[chunk]
                size = acc.shape[1] >> (stage + 1)
                keep = pl.ds(region(chunk, stage + 1), size)
                landed = got.at[layer, pl.ds(acc.shape[1] - 2 * size, size)]
                total = acc[layer, keep, :].astype(jnp.float32) + landed[...].astype(jnp.float32)
                if stage < levels - 1:
                    acc[layer, keep, :] = total.astype(jnp.bfloat16)
                else:
                    res[layer, keep, :] = (total * (1.0 / replicas)).astype(jnp.bfloat16)
            if stage < 2 * levels - 1:
                row_copy(chunk, stage + 1).start()

    def region(chunk, depth):
        acc, _, _, _, order = chunks[chunk]
        start = 0
        for k in range(depth):
            start = start + own_bit[order[k]] * (acc.shape[1] >> (k + 1))
        return pl.multiple_of(start, acc.shape[1] >> depth) if depth else 0

    def row_copy(chunk, stage):
        acc, got, res, layer, order = chunks[chunk]
        rows = acc.shape[1]
        if stage < levels:
            bit = order[stage]
            size = rows >> (stage + 1)
            away = region(chunk, stage) + (1 - own_bit[bit]) * size
            src = acc.at[layer, pl.ds(pl.multiple_of(away, size), size)]
            dst = got.at[layer, pl.ds(rows - 2 * size, size)]
        else:
            depth = 2 * levels - stage
            bit = order[depth - 1]
            part = pl.ds(region(chunk, depth), rows >> depth)
            src = dst = res.at[layer, part]
        index = chunk * 2 * levels + stage
        return pltpu.make_async_remote_copy(
            src_ref=src, dst_ref=dst,
            send_sem=row_send.at[index], recv_sem=row_recv.at[index],
            device_id={"row": row_peer[bit]}, device_id_type=MESH,
        )

    def step(last):
        if last:
            wdl[...] = wd[...]
            wul[...] = wu[...]
            start(range(first))
        x1[...] = forward(0, x0_ref[...], x0_ref[...].astype(jnp.float32))
        outcome = forward(1, x1[...], x1[...].astype(jnp.float32))
        gr[...] = outcome.astype(jnp.float32) - tg_ref[...].astype(jnp.float32)

        def first_work():
            update_up(1, last)
            if last:
                advance(0)

        partial_act = dot_nt(gr[...].astype(jnp.bfloat16), wu[1]) * r_scale
        exchange(0, partial_act, None, first_work)
        row_dot = low_grads(1)
        through = dot_nt(low[...], wd[1]) * d_scale
        coefficient = row_dot * inv[1] * inv[1] / full
        gr[...] = gr[...] + through - coefficient * x1[...].astype(jnp.float32)

        def work():
            update(wd, md, 1, dot_nn(x1[...].T, low[...]) * d_scale, last)
            update_up(0, last)
            if last:
                mul[...] = mu[...].astype(jnp.bfloat16)
                mdl[1] = md[1].astype(jnp.bfloat16)
                start(range(first, len(chunks) - 1))
                advance(1)

        partial_act = dot_nt(gr[...].astype(jnp.bfloat16), wu[0]) * r_scale
        exchange(1, partial_act, None, work)
        low_grads(0)
        update(wd, md, 0, dot_nn(xt[...], low[...]) * d_scale, last)

    def middle(index, carry):
        step(False)
        return carry

    xt[...] = x0_ref[...].T
    lax.fori_loop(0, STEPS - 1, middle, 0)
    step(True)
    mdl[0] = md[0].astype(jnp.bfloat16)
    if not levels:
        wd_out[...] = wd[...]
        wu_out[...] = wu[...]
        md_out[...] = mdl[...]
        mu_out[...] = mul[...]
        return
    start([len(chunks) - 1])
    for slot in range(2, len(chunks) + 2 * levels - 1):
        advance(slot)
    for chunk in range(len(chunks)):
        for stage in range(2 * levels):
            row_copy(chunk, stage).wait_send()

    def stepped(weights, moments):
        moved = weights.astype(jnp.float32) - learn_rate * moments.astype(jnp.float32)
        return moved.astype(jnp.bfloat16)

    wd_out[...] = stepped(res_wd[...], res_md[...])
    wu_out[...] = stepped(res_wu[...], res_mu[...])
    md_out[...] = res_md[...]
    mu_out[...] = res_mu[...]


def fused(shards, replicas, hidden, target, w_down, w_up, m_down, m_up):
    tok, width = hidden.shape
    layers, _, rank = w_down.shape
    half = tok // 2
    hops = shards // 2 - 1
    bf, f32 = jnp.bfloat16, jnp.float32
    vmem = pl.BlockSpec(memory_space=pltpu.VMEM)
    sems = 2 + 2 * hops
    row_sems = max(1, 4 * layers * 2 * len(row_bits(replicas, width, rank)))
    return pl.pallas_call(
        functools.partial(fused_kernel, shards, replicas),
        out_shape=[
            jax.ShapeDtypeStruct(w_down.shape, bf),
            jax.ShapeDtypeStruct(w_up.shape, bf),
            jax.ShapeDtypeStruct(m_down.shape, bf),
            jax.ShapeDtypeStruct(m_up.shape, bf),
        ],
        in_specs=[vmem] * 6,
        out_specs=[vmem] * 4,
        scratch_shapes=[
            pltpu.VMEM(w_down.shape, bf),
            pltpu.VMEM(w_up.shape, bf),
            pltpu.VMEM(m_down.shape, f32),
            pltpu.VMEM(m_up.shape, f32),
            pltpu.VMEM(w_down.shape, bf),
            pltpu.VMEM(w_up.shape, bf),
            pltpu.VMEM(m_down.shape, bf),
            pltpu.VMEM(m_up.shape, bf),
            pltpu.VMEM(w_down.shape, bf),
            pltpu.VMEM(w_up.shape, bf),
            pltpu.VMEM(m_down.shape, bf),
            pltpu.VMEM(m_up.shape, bf),
            pltpu.VMEM(w_down.shape, bf),
            pltpu.VMEM(w_up.shape, bf),
            pltpu.VMEM(m_down.shape, bf),
            pltpu.VMEM(m_up.shape, bf),
            pltpu.SemaphoreType.DMA((row_sems,)),
            pltpu.SemaphoreType.DMA((row_sems,)),
            pltpu.VMEM((tok, width), bf),
            pltpu.VMEM((width, tok), bf),
            pltpu.VMEM((tok, width), f32),
            pltpu.VMEM((layers, tok, rank), f32),
            pltpu.VMEM((layers, tok, rank), bf),
            pltpu.VMEM((layers, tok, 1), f32),
            pltpu.VMEM((tok, rank), f32),
            pltpu.VMEM((tok, 1), f32),
            pltpu.VMEM((tok, rank), bf),
            pltpu.VMEM((half, rank), bf),
            pltpu.VMEM((half, rank), bf),
            pltpu.VMEM((half, rank), bf),
            pltpu.VMEM((2 * hops, half, rank), bf),
            pltpu.VMEM((half, rank), bf),
            pltpu.VMEM((half, rank), bf),
            pltpu.VMEM((8, half), f32),
            pltpu.VMEM((8, half), f32),
            pltpu.VMEM((8, half), f32),
            pltpu.VMEM((2 * hops, 8, half), f32),
            pltpu.VMEM((8, half), f32),
            pltpu.VMEM((8, half), f32),
            pltpu.SemaphoreType.DMA((sems,)),
            pltpu.SemaphoreType.DMA((sems,)),
            pltpu.SemaphoreType.DMA((sems,)),
            pltpu.SemaphoreType.DMA((sems,)),
        ],
        compiler_params=pltpu.CompilerParams(
            collective_id=0, has_side_effects=True, vmem_limit_bytes=60 * 1024 * 1024
        ),
    )(hidden, target, w_down, w_up, m_down, m_up)


def body(shards, replicas, hidden, target, w_down, w_up, m_down, m_up):
    means = fused(
        shards, replicas, hidden[0], target[0], w_down[0], w_up[0], m_down[0], m_up[0]
    )
    if not row_bits(replicas, hidden.shape[2], w_down.shape[3]):
        totals = lax.psum(tuple(means), "row")
        means = [total.astype(jnp.float32) / replicas for total in totals]
    return (
        means[0].astype(jnp.bfloat16),
        means[1].astype(jnp.bfloat16),
        means[2].astype(jnp.float32),
        means[3].astype(jnp.float32),
    )


def solution(mesh):
    placed = (
        P("row", None, "ta"),
        P("row", None, "ta"),
        P("row", None, "ta", None),
        P("row", None, None, "ta"),
        P("row", None, "ta", None),
        P("row", None, None, "ta"),
    )
    return jax.shard_map(
        functools.partial(body, mesh.shape["ta"], mesh.shape["row"]),
        mesh=mesh,
        in_specs=placed,
        out_specs=(
            P(None, "ta", None),
            P(None, None, "ta"),
            P(None, "ta", None),
            P(None, None, "ta"),
        ),
        check_vma=False,
    )
```

```python
import functools

import jax
import jax.numpy as jnp
from jax import lax
from jax.experimental import pallas as pl
from jax.experimental.pallas import tpu as pltpu
from jax.sharding import PartitionSpec as P

MESH = pl.DeviceIdType.MESH
STEPS = 4
norm_eps = 1e-06
learn_rate = 0.02
moment_decay = 0.9


def dot_nn(a, b):
    return jnp.dot(a, b, preferred_element_type=jnp.float32)


def dot_nt(a, b):
    return lax.dot_general(a, b, (((1,), (1,)), ((), ())), preferred_element_type=jnp.float32)


def row_bits(replicas, *lengths):
    if replicas & (replicas - 1) or any(length % (16 * replicas) for length in lengths):
        return []
    return [2**k for k in range(replicas.bit_length() - 1)]


def fused_kernel(
    shards, replicas,
    x0_ref, tg_ref, wd_in, wu_in, md_in, mu_in,
    wd_out, wu_out, md_out, mu_out,
    wd, wu, md, mu, wdl, wul, mdl, mul, res_wd, res_wu, res_md, res_mu,
    got_wd, got_wu, got_md, got_mu, row_send, row_recv,
    x1, xt, gr, pre, act, inv, tot, sqs, low,
    s1, r1, s2, r2, s3, r3, q1, p1, q2, p2, q3, p3,
    main_send, main_recv, side_send, side_recv,
):
    tok, width = x0_ref.shape
    rank = wd.shape[2]
    full = width * shards
    half = tok // 2
    chips = shards // 2
    me = lax.axis_index("ta")
    core = lax.rem(me, 2)
    sibling = me + 1 - 2 * core
    partners = [lax.rem(me + 2 * k, shards) for k in range(1, chips)]
    d_scale = full ** (-0.5)
    r_scale = rank ** (-0.5)

    barrier = pltpu.get_barrier_semaphore()
    for peer in [sibling] + partners:
        pl.semaphore_signal(barrier, inc=1, device_id={"ta": peer}, device_id_type=MESH)
    bits = row_bits(replicas, width, rank)
    levels = len(bits)
    spot = lax.axis_index("row")
    own_bit = {bit: lax.rem(spot // bit, 2) for bit in bits}
    row_peer = {bit: spot + bit - 2 * bit * own_bit[bit] for bit in bits}
    for bit in bits:
        pl.semaphore_signal(barrier, inc=1, device_id={"row": row_peer[bit]}, device_id_type=MESH)
    pl.semaphore_wait(barrier, chips + levels)

    wd[...] = wd_in[...]
    wu[...] = wu_in[...]
    md[...] = md_in[...]
    mu[...] = mu_in[...]

    mine = pl.ds(pl.multiple_of(core * half, half), half)
    other = pl.ds(pl.multiple_of((1 - core) * half, half), half)

    def send(src, dst, sems, index, peer):
        copy = pltpu.make_async_remote_copy(
            src_ref=src, dst_ref=dst,
            send_sem=sems[0].at[index], recv_sem=sems[1].at[index],
            device_id={"ta": peer}, device_id_type=MESH,
        )
        copy.start()
        return copy

    main = (main_send, main_recv)
    side = (side_send, side_recv)

    def to_row(column):
        return jnp.broadcast_to(column, (half, half)).T[0:8]

    def to_column(row):
        return jnp.broadcast_to(row[0:1, :], (half, half)).T[:, 0:1]

    def exchange(parity, value, squares, work):
        tot[...] = value
        s1[...] = tot[other, :].astype(jnp.bfloat16)
        copies = [send(s1, r1, main, 0, sibling)]
        if squares is not None:
            sqs[...] = squares
            q1[...] = to_row(sqs[other, :])
            copies.append(send(q1, p1, side, 0, sibling))
            own_row = to_row(sqs[mine, :])
        for copy in copies:
            copy.wait()
        pair = tot[mine, :] + r1[...].astype(jnp.float32)
        s2[...] = pair.astype(jnp.bfloat16)
        base = parity * (chips - 1)
        copies = [
            send(s2, r2.at[base + k], main, 1 + base + k, peer) for k, peer in enumerate(partners)
        ]
        if squares is not None:
            pair_row = own_row + p1[...]
            q2[...] = pair_row
            copies += [
                send(q2, p2.at[base + k], side, 1 + base + k, peer)
                for k, peer in enumerate(partners)
            ]
        if work is not None:
            work()
        for copy in copies:
            copy.wait()
        total = pair
        for k in range(chips - 1):
            total = total + r2[base + k].astype(jnp.float32)
        last = 1 + 2 * (chips - 1)
        s3[...] = total.astype(jnp.bfloat16)
        copies = [send(s3, r3, main, last, sibling)]
        tot[mine, :] = total
        if squares is not None:
            row = pair_row
            for k in range(chips - 1):
                row = row + p2[base + k]
            q3[...] = row
            copies.append(send(q3, p3, side, last, sibling))
            sqs[mine, :] = to_column(row)
        for copy in copies:
            copy.wait()
        tot[other, :] = r3[...].astype(jnp.float32)
        if squares is not None:
            sqs[other, :] = to_column(p3[...])

    def forward(layer, rows, wide_rows, work=None):
        squares = jnp.sum(wide_rows * wide_rows, axis=1, keepdims=True)
        exchange(layer, dot_nn(rows, wd[layer]) * d_scale, squares, work)
        inverse = lax.rsqrt(sqs[...] / full + norm_eps)
        preact = tot[...] * inverse
        activation = (preact * jax.nn.sigmoid(preact)).astype(jnp.bfloat16)
        inv[layer] = inverse
        pre[layer] = preact
        act[layer] = activation
        lifted = dot_nn(activation, wu[layer]) * r_scale
        return (wide_rows + lifted).astype(jnp.bfloat16)

    def update(w, m, layer, grad, last):
        moment = moment_decay * m[layer] + grad
        m[layer] = moment
        if last and levels:
            return
        w[layer] = (w[layer].astype(jnp.float32) - learn_rate * moment).astype(jnp.bfloat16)

    def update_up(layer, last):
        update(wu, mu, layer, dot_nn(act[layer].T, gr[...].astype(jnp.bfloat16)) * r_scale, last)

    def low_grads(layer):
        preact = pre[layer]
        sig = jax.nn.sigmoid(preact)
        grad_pre = tot[...] * (sig * (1.0 + preact * (1.0 - sig)))
        low[...] = (grad_pre * inv[layer]).astype(jnp.bfloat16)
        return jnp.sum(grad_pre * preact, axis=1, keepdims=True)

    down, up = (wdl, got_wd, res_wd), (wul, got_wu, res_wu)
    mdown, mup = (mdl, got_md, res_md), (mul, got_mu, res_mu)
    layers = list(reversed(range(wd.shape[0])))
    chunks = [pair + (layer, bits) for layer in layers for pair in (up, down)]
    first = len(chunks)
    swapped = bits[:2][::-1] + bits[2:]
    chunks += [
        pair + (layer, swapped if layer == 0 and pair is mup else bits)
        for layer in layers
        for pair in (mup, mdown)
    ]

    def start(picked):
        for chunk in picked if levels else []:
            row_copy(chunk, 0).start()

    def advance(slot):
        for chunk in range(len(chunks)):
            stage = slot - chunk
            if not levels or stage < 0 or stage >= 2 * levels:
                continue
            row_copy(chunk, stage).wait_recv()
            if stage < levels:
                acc, got, res, layer, order = chunks[chunk]
                size = acc.shape[1] >> (stage + 1)
                keep = pl.ds(region(chunk, stage + 1), size)
                landed = got.at[layer, pl.ds(acc.shape[1] - 2 * size, size)]
                total = acc[layer, keep, :].astype(jnp.float32) + landed[...].astype(jnp.float32)
                if stage < levels - 1:
                    acc[layer, keep, :] = total.astype(jnp.bfloat16)
                else:
                    res[layer, keep, :] = (total * (1.0 / replicas)).astype(jnp.bfloat16)
            if stage < 2 * levels - 1:
                row_copy(chunk, stage + 1).start()

    def region(chunk, depth):
        acc, _, _, _, order = chunks[chunk]
        start = 0
        for k in range(depth):
            start = start + own_bit[order[k]] * (acc.shape[1] >> (k + 1))
        return pl.multiple_of(start, acc.shape[1] >> depth) if depth else 0

    def row_copy(chunk, stage):
        acc, got, res, layer, order = chunks[chunk]
        rows = acc.shape[1]
        if stage < levels:
            bit = order[stage]
            size = rows >> (stage + 1)
            away = region(chunk, stage) + (1 - own_bit[bit]) * size
            src = acc.at[layer, pl.ds(pl.multiple_of(away, size), size)]
            dst = got.at[layer, pl.ds(rows - 2 * size, size)]
        else:
            depth = 2 * levels - stage
            bit = order[depth - 1]
            part = pl.ds(region(chunk, depth), rows >> depth)
            src = dst = res.at[layer, part]
        index = chunk * 2 * levels + stage
        return pltpu.make_async_remote_copy(
            src_ref=src, dst_ref=dst,
            send_sem=row_send.at[index], recv_sem=row_recv.at[index],
            device_id={"row": row_peer[bit]}, device_id_type=MESH,
        )

    def step(last):
        if last:
            wdl[...] = wd[...]
            wul[...] = wu[...]
            start(range(first))
        x1[...] = forward(0, x0_ref[...], x0_ref[...].astype(jnp.float32))
        outcome = forward(
            1, x1[...], x1[...].astype(jnp.float32), (lambda: advance(0)) if last else None
        )
        gr[...] = outcome.astype(jnp.float32) - tg_ref[...].astype(jnp.float32)

        def first_work():
            update_up(1, last)
            if last:
                advance(1)

        partial_act = dot_nt(gr[...].astype(jnp.bfloat16), wu[1]) * r_scale
        exchange(0, partial_act, None, first_work)
        row_dot = low_grads(1)
        through = dot_nt(low[...], wd[1]) * d_scale
        coefficient = row_dot * inv[1] * inv[1] / full
        gr[...] = gr[...] + through - coefficient * x1[...].astype(jnp.float32)

        def work():
            update(wd, md, 1, dot_nn(x1[...].T, low[...]) * d_scale, last)
            update_up(0, last)
            if last:
                mul[...] = mu[...].astype(jnp.bfloat16)
                mdl[1] = md[1].astype(jnp.bfloat16)
                start(range(first, len(chunks) - 1))
                advance(2)

        partial_act = dot_nt(gr[...].astype(jnp.bfloat16), wu[0]) * r_scale
        exchange(1, partial_act, None, work)
        low_grads(0)
        update(wd, md, 0, dot_nn(xt[...], low[...]) * d_scale, last)

    def middle(index, carry):
        step(False)
        return carry

    xt[...] = x0_ref[...].T
    lax.fori_loop(0, STEPS - 1, middle, 0)
    step(True)
    mdl[0] = md[0].astype(jnp.bfloat16)
    if not levels:
        wd_out[...] = wd[...]
        wu_out[...] = wu[...]
        md_out[...] = mdl[...]
        mu_out[...] = mul[...]
        return
    start([len(chunks) - 1])
    for slot in range(3, len(chunks) + 2 * levels - 1):
        advance(slot)
    for chunk in range(len(chunks)):
        for stage in range(2 * levels):
            row_copy(chunk, stage).wait_send()

    def stepped(weights, moments):
        moved = weights.astype(jnp.float32) - learn_rate * moments.astype(jnp.float32)
        return moved.astype(jnp.bfloat16)

    wd_out[...] = stepped(res_wd[...], res_md[...])
    wu_out[...] = stepped(res_wu[...], res_mu[...])
    md_out[...] = res_md[...]
    mu_out[...] = res_mu[...]


def fused(shards, replicas, hidden, target, w_down, w_up, m_down, m_up):
    tok, width = hidden.shape
    layers, _, rank = w_down.shape
    half = tok // 2
    hops = shards // 2 - 1
    bf, f32 = jnp.bfloat16, jnp.float32
    vmem = pl.BlockSpec(memory_space=pltpu.VMEM)
    sems = 2 + 2 * hops
    row_sems = max(1, 4 * layers * 2 * len(row_bits(replicas, width, rank)))
    return pl.pallas_call(
        functools.partial(fused_kernel, shards, replicas),
        out_shape=[
            jax.ShapeDtypeStruct(w_down.shape, bf),
            jax.ShapeDtypeStruct(w_up.shape, bf),
            jax.ShapeDtypeStruct(m_down.shape, bf),
            jax.ShapeDtypeStruct(m_up.shape, bf),
        ],
        in_specs=[vmem] * 6,
        out_specs=[vmem] * 4,
        scratch_shapes=[
            pltpu.VMEM(w_down.shape, bf),
            pltpu.VMEM(w_up.shape, bf),
            pltpu.VMEM(m_down.shape, f32),
            pltpu.VMEM(m_up.shape, f32),
            pltpu.VMEM(w_down.shape, bf),
            pltpu.VMEM(w_up.shape, bf),
            pltpu.VMEM(m_down.shape, bf),
            pltpu.VMEM(m_up.shape, bf),
            pltpu.VMEM(w_down.shape, bf),
            pltpu.VMEM(w_up.shape, bf),
            pltpu.VMEM(m_down.shape, bf),
            pltpu.VMEM(m_up.shape, bf),
            pltpu.VMEM(w_down.shape, bf),
            pltpu.VMEM(w_up.shape, bf),
            pltpu.VMEM(m_down.shape, bf),
            pltpu.VMEM(m_up.shape, bf),
            pltpu.SemaphoreType.DMA((row_sems,)),
            pltpu.SemaphoreType.DMA((row_sems,)),
            pltpu.VMEM((tok, width), bf),
            pltpu.VMEM((width, tok), bf),
            pltpu.VMEM((tok, width), f32),
            pltpu.VMEM((layers, tok, rank), f32),
            pltpu.VMEM((layers, tok, rank), bf),
            pltpu.VMEM((layers, tok, 1), f32),
            pltpu.VMEM((tok, rank), f32),
            pltpu.VMEM((tok, 1), f32),
            pltpu.VMEM((tok, rank), bf),
            pltpu.VMEM((half, rank), bf),
            pltpu.VMEM((half, rank), bf),
            pltpu.VMEM((half, rank), bf),
            pltpu.VMEM((2 * hops, half, rank), bf),
            pltpu.VMEM((half, rank), bf),
            pltpu.VMEM((half, rank), bf),
            pltpu.VMEM((8, half), f32),
            pltpu.VMEM((8, half), f32),
            pltpu.VMEM((8, half), f32),
            pltpu.VMEM((2 * hops, 8, half), f32),
            pltpu.VMEM((8, half), f32),
            pltpu.VMEM((8, half), f32),
            pltpu.SemaphoreType.DMA((sems,)),
            pltpu.SemaphoreType.DMA((sems,)),
            pltpu.SemaphoreType.DMA((sems,)),
            pltpu.SemaphoreType.DMA((sems,)),
        ],
        compiler_params=pltpu.CompilerParams(
            collective_id=0, has_side_effects=True, vmem_limit_bytes=60 * 1024 * 1024
        ),
    )(hidden, target, w_down, w_up, m_down, m_up)


def body(shards, replicas, hidden, target, w_down, w_up, m_down, m_up):
    means = fused(
        shards, replicas, hidden[0], target[0], w_down[0], w_up[0], m_down[0], m_up[0]
    )
    if not row_bits(replicas, hidden.shape[2], w_down.shape[3]):
        totals = lax.psum(tuple(means), "row")
        means = [total.astype(jnp.float32) / replicas for total in totals]
    return (
        means[0].astype(jnp.bfloat16),
        means[1].astype(jnp.bfloat16),
        means[2].astype(jnp.float32),
        means[3].astype(jnp.float32),
    )


def solution(mesh):
    placed = (
        P("row", None, "ta"),
        P("row", None, "ta"),
        P("row", None, "ta", None),
        P("row", None, None, "ta"),
        P("row", None, "ta", None),
        P("row", None, None, "ta"),
    )
    return jax.shard_map(
        functools.partial(body, mesh.shape["ta"], mesh.shape["row"]),
        mesh=mesh,
        in_specs=placed,
        out_specs=(
            P(None, "ta", None),
            P(None, None, "ta"),
            P(None, "ta", None),
            P(None, None, "ta"),
        ),
        check_vma=False,
    )
```
